32 devices in a mesh: dp: 8 (over z, y), tensor: 4 (over x, core).
Axes of the slice: x: 2, y: 2, z: 4, core: 2. Of those that a mesh axis runs over, the one named last changes fastest.
Arguments:
- acts: bfloat16 [8, 2048, 1024], P('dp', 'tensor'), may hold values from -6 to 6
- grad_out: bfloat16 [8, 2048, 1024], P('dp', 'tensor'), may hold values from -6 to 6
- norm_gain: float32 [1024], replicated, may hold values from 0.5 to 1.5
- w_zx: bfloat16 [1024, 2, 2048], P('dp', None, 'tensor'), may hold values from -0.1875 to 0.1875
- w_bc: bfloat16 [1024, 256], P('dp'), may hold values from -0.1875 to 0.1875
- w_dt: bfloat16 [1024, 32], P('dp', 'tensor'), may hold values from -0.1875 to 0.1875
- w_out: bfloat16 [1024, 2048], P('dp', 'tensor'), may hold values from -0.125 to 0.125
- conv_x: float32 [4, 2048], replicated, may hold values from -3 to 3
- conv_x_bias: float32 [2048], replicated, may hold values from -0.5 to 0.5
- conv_bc: float32 [4, 256], replicated, may hold values from -3 to 3
- conv_bc_bias: float32 [256], replicated, may hold values from -0.5 to 0.5
- dt_bias: float32 [32], replicated, may hold values from -7 to -2
- a_log: float32 [32], replicated, may hold values from 0 to 2.77
- d_skip: float32 [32], replicated, may hold values from 0.5 to 1.5
- gate_gain: float32 [2048], replicated, may hold values from 0.5 to 1.5
Outputs:
- out_acts: bfloat16 [8, 2048, 1024], P('dp', 'tensor')
- grad_acts: float32 [8, 2048, 1024], P('dp', 'tensor')
- grad_norm_gain: float32 [1024], replicated
- grad_w_zx: float32 [1024, 2, 2048], P('dp', None, 'tensor')
- grad_w_bc: float32 [1024, 256], P('dp')
- grad_w_dt: float32 [1024, 32], P('dp', 'tensor')
- grad_w_out: float32 [1024, 2048], P('dp', 'tensor')
- grad_conv_x: float32 [4, 2048], replicated
- grad_conv_x_bias: float32 [2048], replicated
- grad_conv_bc: float32 [4, 256], replicated
- grad_conv_bc_bias: float32 [256], replicated
- grad_dt_bias: float32 [32], replicated
- grad_a_log: float32 [32], replicated
- grad_d_skip: float32 [32], replicated
- grad_gate_gain: float32 [2048], replicated
The draws below stay inside these ranges and needn't reach their ends.
All inputs are finite; a program needn't handle non-finite values.
Results may differ from the reference program's by a relative error of at most 0.0096.
Values may be sent and summed in bfloat16 or wider, within the bound.
A program may use at most 192 MiB of HBM per device.

```python
import jax
import jax.numpy as jnp
from jax import lax

D = 1024
DI = 2048
H = 32
N = 128
K = 4
BLOCK_LEN = 256
SEQ = 2048
BATCH = 8


def spiked(values, key, source, target, shards_of, factor):
    def block_of(axis_at):
        return (jnp.arange(values.shape[axis_at]) // (values.shape[axis_at] // shards_of)).reshape((-1,) + (1,) * (values.ndim - 1 - axis_at))

    near = jax.random.permutation(key, shards_of)[block_of(target)]
    other_side = (block_of(target) + shards_of // 2) % shards_of
    return jnp.where((block_of(source) == near) | (block_of(source) == other_side), factor * values, values)


def block_levels(key, extent, pieces, smallest, top_value):
    def one(dim, parts):
        heights = jax.random.uniform(jax.random.fold_in(jax.random.fold_in(key, 6), dim), (parts,), jnp.float32, smallest / len(pieces), top_value / len(pieces))
        return jnp.repeat(jnp.exp(heights), extent[dim] // parts).reshape((-1,) + (1,) * (len(extent) - dim - 1))

    gain = one(*pieces[0])
    for cut in pieces[1:]:
        gain = gain * one(*cut)
    return gain


def bell_draw(stream_key, extent, scale, most, pieces=(), held_as=jnp.bfloat16):
    values = jax.random.normal(stream_key, extent, jnp.float32) * scale
    if len(pieces) > 0:
        values = block_levels(stream_key, extent, pieces, -0.22, 0.18) * values
    return jnp.clip(values, min=-most, max=most).astype(held_as)


def noise_with(key, shape, scale, bound, shards, heavy, held_as=jnp.bfloat16):
    values = scale * jax.random.normal(key, shape, jnp.float32)
    if shards:
        values = values * block_levels(key, shape, shards, -0.22, 0.18)
    return jnp.clip(spiked(values, jax.random.fold_in(key, 3), *heavy), -bound, bound).astype(held_as)


def setup_inputs(seed: int = 0) -> dict:
    seeds = jax.random.split(jax.random.key(seed), 16)
    return {
        "acts": noise_with(seeds[0], (BATCH, SEQ, D), 1.0, 6.0, ((0, 8), (1, 4)), (0, 2, 8, 2.0)),
        "grad_out": noise_with(seeds[1], (BATCH, SEQ, D), 1.0, 6.0, ((0, 8), (1, 4)), (0, 2, 8, 2.0)),
        "norm_gain": jnp.clip(1.0 + 0.1 * jax.random.normal(seeds[2], (D,), jnp.float32), 0.5, 1.5),
        "w_zx": bell_draw(seeds[3], (D, 2, DI), D ** -0.5, 0.1875, ((0, 8), (2, 4))),
        "w_bc": bell_draw(seeds[4], (D, 2 * N), D ** -0.5, 0.1875, ((0, 8),)),
        "w_dt": bell_draw(seeds[5], (D, H), D ** -0.5, 0.1875, ((0, 8), (1, 4))),
        "w_out": bell_draw(seeds[6], (D, DI), DI ** -0.5, 0.125, ((0, 8), (1, 4))),
        "conv_x": bell_draw(seeds[7], (K, DI), 0.5, 3.0, (), jnp.float32),
        "conv_x_bias": jnp.clip(jax.random.uniform(seeds[8], (DI,), jnp.float32, -0.5, 0.5), -0.5, 0.5),
        "conv_bc": bell_draw(seeds[9], (K, 2 * N), 0.5, 3.0, (), jnp.float32),
        "conv_bc_bias": jnp.clip(jax.random.uniform(seeds[10], (2 * N,), jnp.float32, -0.5, 0.5), -0.5, 0.5),
        "dt_bias": jnp.clip(jax.random.uniform(seeds[11], (H,), jnp.float32, -7.0, -2.0), -7.0, -2.0),
        "a_log": jnp.clip(jax.random.uniform(seeds[12], (H,), jnp.float32, 0.0, 2.77), 0.0, 2.77),
        "d_skip": jnp.clip(jax.random.uniform(seeds[13], (H,), jnp.float32, 0.5, 1.5), 0.5, 1.5),
        "gate_gain": jnp.clip(1.0 + 0.1 * jax.random.normal(seeds[14], (DI,), jnp.float32), 0.5, 1.5),
    }


EPSILON = 1e-05
FULL_PRECISION = lax.Precision.HIGHEST

@jax.custom_vjp
def low(v):
    return lax.optimization_barrier(v.astype(jnp.bfloat16)).astype(jnp.float32)

@jax.custom_vjp
def low_back(v):
    return v

def low_keep(v):
    return (low(v), None)

def low_pass(kept, grad):
    return (grad,)

def back_keep(v):
    return (v, None)

def back_low(kept, grad):
    return (low(grad),)
low.defvjp(low_keep, low_pass)
low_back.defvjp(back_keep, back_low)

def causal_conv(values, conv_taps):
    tap_count = conv_taps.shape[0]
    length = values.shape[0]
    padded = jnp.pad(values, ((tap_count - 1, 0), (0, 0)))
    result = conv_taps[0] * padded[0:length]
    for offset in range(1, tap_count):
        result = result + conv_taps[offset] * padded[offset:offset + length]
    return result

def ssd_scan(x_heads, step_dt, decay_rate, b_mat, c_mat, block_size):
    length, head_count, head_width = x_heads.shape
    state_count = b_mat.shape[1]
    block_count = length // block_size
    x_blocks = x_heads.reshape(block_count, block_size, head_count, head_width)
    dt_blocks = step_dt.reshape(block_count, block_size, head_count)
    b_blocks = b_mat.reshape(block_count, block_size, state_count)
    c_blocks = c_mat.reshape(block_count, block_size, state_count)
    positions = jnp.arange(block_size)
    causal_mask = (positions[:, None] >= positions[None, :]).astype(jnp.float32)

    def step_block(state, inputs):
        x_block, dt_block, b_block, c_block = inputs
        cum_logs = jnp.cumsum(dt_block * decay_rate[None, :], axis=0)
        scores = jnp.dot(c_block, b_block.T, precision=FULL_PRECISION)
        log_gaps = (cum_logs[:, None, :] - cum_logs[None, :, :]) * causal_mask[:, :, None]
        weights = scores[:, :, None] * jnp.exp(log_gaps) * causal_mask[:, :, None] * dt_block[None, :, :]
        within = jnp.einsum('ijh,jhp->ihp', weights, x_block, precision=FULL_PRECISION)
        carried = jnp.einsum('in,hpn->ihp', c_block, state, precision=FULL_PRECISION) * jnp.exp(cum_logs)[:, :, None]
        block_total = cum_logs[-1]
        state_weight = jnp.exp(block_total[None, :] - cum_logs) * dt_block
        update = jnp.einsum('jhp,jn->hpn', x_block * state_weight[:, :, None], b_block, precision=FULL_PRECISION)
        new_state = state * jnp.exp(block_total)[:, None, None] + update
        return (new_state, within + carried)
    zero_state = jnp.zeros((head_count, head_width, state_count), jnp.float32)
    final_state, outputs = lax.scan(jax.checkpoint(step_block), zero_state, (x_blocks, dt_blocks, b_blocks, c_blocks))
    return outputs.reshape(length, head_count, head_width)

def layer(acts_row, params):
    norm_gain, w_zx, w_bc, w_dt, w_out, conv_x, conv_x_bias, conv_bc, conv_bc_bias, dt_bias, a_log, d_skip, gate_gain = params
    length = acts_row.shape[0]
    head_count = w_dt.shape[1]
    state_count = w_bc.shape[1] // 2
    normed_in = acts_row * lax.rsqrt(lax.optimization_barrier(jnp.mean(acts_row * acts_row, axis=-1, keepdims=True)) + EPSILON) * norm_gain
    hidden = low(normed_in)
    gate_in = low_back(jnp.dot(hidden, w_zx[:, 0, :], precision=FULL_PRECISION))
    x_in = low_back(jnp.dot(hidden, w_zx[:, 1, :], precision=FULL_PRECISION))
    bc_in = low_back(jnp.dot(hidden, w_bc, precision=FULL_PRECISION))
    dt_in = low_back(jnp.dot(hidden, w_dt, precision=FULL_PRECISION))
    x_conv = jax.nn.silu(causal_conv(x_in, conv_x) + conv_x_bias)
    bc_conv = jax.nn.silu(causal_conv(bc_in, conv_bc) + conv_bc_bias)
    x_heads = low(x_conv).reshape(length, head_count, -1)
    b_mat = low(bc_conv[:, :state_count])
    c_mat = low(bc_conv[:, state_count:])
    step_dt = jax.nn.softplus(dt_in + dt_bias)
    decay_rate = -jnp.exp(a_log)
    mixed = ssd_scan(x_heads, step_dt, decay_rate, b_mat, c_mat, BLOCK_LEN) + d_skip[None, :, None] * x_heads
    gated = mixed.reshape(length, -1) * jax.nn.silu(gate_in)
    normed = gated * lax.rsqrt(lax.optimization_barrier(jnp.mean(gated * gated, axis=-1, keepdims=True)) + EPSILON) * gate_gain
    mixed_out = low_back(low(normed))
    return acts_row + jnp.dot(mixed_out, w_out.T, precision=FULL_PRECISION)

def add_pair(first_item, second_item):
    return first_item + second_item

def reference(acts, grad_out, norm_gain, w_zx, w_bc, w_dt, w_out, conv_x, conv_x_bias, conv_bc, conv_bc_bias, dt_bias, a_log, d_skip, gate_gain):
    params = tuple((item.astype(jnp.float32) for item in (norm_gain, w_zx, w_bc, w_dt, w_out, conv_x, conv_x_bias, conv_bc, conv_bc_bias, dt_bias, a_log, d_skip, gate_gain)))

    def one_sequence(totals, inputs):
        acts_row, grad_row = inputs
        result, backward = jax.vjp(layer, acts_row.astype(jnp.float32), params)
        grad_input, grad_params = backward(grad_row.astype(jnp.float32))
        totals = jax.tree.map(add_pair, totals, grad_params)
        return (totals, (result.astype(jnp.bfloat16), grad_input))
    zero_totals = jax.tree.map(jnp.zeros_like, params)
    totals, outputs = lax.scan(one_sequence, zero_totals, (acts, grad_out))
    out_acts, grad_acts = outputs
    return (out_acts, grad_acts, totals[0], totals[1], totals[2], totals[3], totals[4], totals[5], totals[6], totals[7], totals[8], totals[9], totals[10], totals[11], totals[12])
```

```python
import functools

import jax
import jax.numpy as jnp
from jax import lax
from jax.experimental import pallas as pl
from jax.experimental.pallas import tpu as pltpu
from jax.sharding import PartitionSpec as P

EPSILON = 1e-05
F32, BF16 = jnp.float32, jnp.bfloat16
CHUNK = 128
STEP = 256
LANES = 128
FAR = -1e30
NN = (((1,), (0,)), ((), ()))
NT = (((1,), (1,)), ((), ()))
TN = (((0,), (0,)), ((), ()))


def mm(a, b, dims=NN):
    return lax.dot_general(a, b, dims, preferred_element_type=F32)


def mm_full(a, b, dims=NN):
    return lax.dot_general(
        a, b, dims, preferred_element_type=F32, precision=lax.Precision.HIGHEST
    )


def sigmoid(v):
    return 1.0 / (1.0 + jnp.exp(-v))


def softplus(v):
    u = jnp.exp(-jnp.abs(v))
    small = u * (1.0 - u * (0.5 - u * (1.0 / 3.0)))
    return jnp.maximum(v, 0.0) + jnp.where(u < 1e-2, small, jnp.log(1.0 + u))


def iota(shape, dim):
    return lax.broadcasted_iota(jnp.int32, shape, dim)


def spread(table, pair, half):
    return jnp.where(half, table[:, 2 * pair : 2 * pair + 1], table[:, 2 * pair + 1 : 2 * pair + 2])


def fold_rows(v):
    rows, cols = v.shape
    return jnp.sum(v.reshape(rows // 8, 8, cols), axis=0)


def chunk_rates(dt_in, dt_bias, rate):
    step = softplus(dt_in + dt_bias)
    log_step = step * rate
    lower = (iota((CHUNK, CHUNK), 0) >= iota((CHUNK, CHUNK), 1)).astype(F32)
    cum = mm_full(lower, log_step)
    return step, log_step, cum


def fwd_kernel(
    heads, channels, states,
    hid_ref, w_ref, grad_ref, wout_ref, conv_ref, row_ref, chan_ref,
    proj_ref, pre_ref, mixed_ref, gm_ref, stat_ref, start_ref,
    shift, state,
):
    conv_cols = channels + 2 * states

    @pl.when(pl.program_id(0) == 0)
    def _():
        shift[0:8, :] = jnp.zeros((8, conv_cols), F32)
        state[...] = jnp.zeros_like(state)

    proj = mm(hid_ref[...], w_ref[...])
    proj_ref[...] = proj
    gm_ref[...] = mm(grad_ref[...], wout_ref[...]).astype(BF16)
    conv_in = proj[:, channels : channels + conv_cols]
    shift[8 : 8 + STEP, :] = conv_in
    pre = conv_ref[4:5, :] + conv_ref[3:4, :] * conv_in
    for back in range(1, 4):
        pre = pre + conv_ref[3 - back : 4 - back, :] * shift[8 - back : 8 - back + STEP, :]
    shift[0:8, :] = conv_in[STEP - 8 :, :]
    pre_ref[...] = pre
    half = iota((CHUNK, LANES), 1) < LANES // 2
    lower = iota((CHUNK, CHUNK), 0) >= iota((CHUNK, CHUNK), 1)
    lane = iota((CHUNK, LANES), 1)
    for sub in range(STEP // CHUNK):
        rows = pl.ds(sub * CHUNK, CHUNK)
        pre_c = pre_ref[rows, :]
        act = (pre_c * sigmoid(pre_c)).astype(BF16)
        x_low = act[:, :channels]
        b_mat = act[:, channels : channels + states]
        c_mat = act[:, channels + states :]
        dt_in = proj_ref[rows, channels + conv_cols :]
        step, log_step, cum = chunk_rates(dt_in, row_ref[0:1, :], row_ref[1:2, :])
        cum_t = cum.T
        step_t = step.T
        last = cum[CHUNK - 1 : CHUNK, :]
        grow = jnp.exp(cum)
        tail = jnp.exp(last - cum) * step
        total = jnp.exp(last)
        scores = mm(c_mat, b_mat, NT)
        state_low = state[...].astype(BF16)
        start_ref[sub] = state_low
        from_state = mm(c_mat, state_low, NT)
        square = jnp.zeros((CHUNK, 1), F32)
        dots = jnp.zeros((CHUNK, 1), F32)
        for pair in range(heads // 2):
            cols = slice(pair * LANES, (pair + 1) * LANES)
            x_pair = x_low[:, cols]
            zero = jnp.zeros_like(x_pair)
            parts = []
            for side in range(2):
                head = 2 * pair + side
                gap = jnp.where(lower, cum[:, head : head + 1] - cum_t[head : head + 1, :], FAR)
                parts.append((scores * jnp.exp(gap) * step_t[head : head + 1, :]).astype(BF16))
            x_wide = x_pair.astype(F32)
            both = jnp.concatenate(parts, axis=1)
            x_two = jnp.concatenate(
                [jnp.where(half, x_wide, 0.0).astype(BF16), jnp.where(half, 0.0, x_wide).astype(BF16)],
                axis=0,
            )
            mixed = (
                mm(both, x_two)
                + from_state[:, cols] * spread(grow, pair, half)
                + chan_ref[0:1, cols] * x_wide
            )
            mixed_ref[rows, cols] = mixed
            gate = proj_ref[rows, cols]
            gated = mixed * (gate * sigmoid(gate))
            square = square + jnp.sum(gated * gated, axis=1, keepdims=True)
            gm = gm_ref[rows, cols].astype(F32)
            dots = dots + jnp.sum(gm * chan_ref[1:2, cols] * gated, axis=1, keepdims=True)
            weighted = (x_wide * spread(tail, pair, half)).astype(BF16)
            update = mm(weighted, b_mat, TN)
            for side in range(2):
                head = 2 * pair + side
                place = pl.ds(pair * LANES + side * 64, 64)
                state[place, :] = (
                    state[place, :] * total[:, head : head + 1] + update[side * 64 : side * 64 + 64, :]
                )
        stat = jnp.where(lane == 0, square, jnp.where(lane == 1, dots, 0.0))
        stat_ref[:, sub * CHUNK : (sub + 1) * CHUNK] = stat.T[0:8, :]


def bwd_kernel(
    heads, channels, states, total_channels,
    proj_ref, pre_ref, mixed_ref, gm_ref, stat_ref, start_ref, conv_ref, row_ref, chan_ref,
    mix_out_ref, grad_ref, acc_conv_ref, acc_chan_ref, acc_row_ref,
    later, grad_state,
):
    conv_cols = channels + 2 * states
    dt_at = channels + conv_cols

    @pl.when(pl.program_id(0) == 0)
    def _():
        later[CHUNK : CHUNK + 8, :] = jnp.zeros((8, conv_cols), F32)
        grad_state[...] = jnp.zeros_like(grad_state)
        acc_conv_ref[...] = jnp.zeros_like(acc_conv_ref)
        acc_chan_ref[...] = jnp.zeros_like(acc_chan_ref)
        acc_row_ref[...] = jnp.zeros_like(acc_row_ref)

    half = iota((CHUNK, LANES), 1) < LANES // 2
    upper = iota((CHUNK, CHUNK), 1) >= iota((CHUNK, CHUNK), 0)
    upper_ones = upper.astype(F32)
    lane = iota((CHUNK, LANES), 1)
    chan_head = iota((LANES, LANES), 0) // 64
    for sub in reversed(range(STEP // CHUNK)):
        rows = pl.ds(sub * CHUNK, CHUNK)
        pre_c = pre_ref[rows, :]
        sig_pre = sigmoid(pre_c)
        act_wide = pre_c * sig_pre
        slope = sig_pre * (1.0 + pre_c * (1.0 - sig_pre))
        act = act_wide.astype(BF16)
        b_mat = act[:, channels : channels + states]
        c_mat = act[:, channels + states :]
        dt_raw = proj_ref[rows, dt_at:] + row_ref[0:1, :]
        step, log_step, cum = chunk_rates(proj_ref[rows, dt_at:], row_ref[0:1, :], row_ref[1:2, :])
        cum_t = cum.T
        last = cum[CHUNK - 1 : CHUNK, :]
        grow = jnp.exp(cum)
        fade = jnp.exp(last - cum)
        tail = fade * step
        total = jnp.exp(last)
        stat = jnp.concatenate(
            [stat_ref[:, sub * CHUNK : (sub + 1) * CHUNK], jnp.zeros((CHUNK - 8, CHUNK), F32)], axis=0
        ).T
        inv = lax.rsqrt(stat[:, 0:1] / total_channels + EPSILON)
        pull = inv * inv * inv * (stat[:, 1:2] / total_channels)
        state_low = start_ref[sub]
        grad_low = grad_state[...].astype(BF16)
        scores_t = mm(b_mat, c_mat, NT)
        from_state = mm(c_mat, state_low, NT)
        from_grad = mm(b_mat, grad_low, NT)
        grad_scores = jnp.zeros((CHUNK, CHUNK), F32)
        plain_sum = jnp.zeros((CHUNK, LANES), F32)
        in_sum = jnp.zeros((CHUNK, LANES), F32)
        out_sum = jnp.zeros((CHUNK, LANES), F32)
        row_parts = []
        const_row = jnp.zeros((1, LANES), F32)
        lane_row = iota((1, LANES), 1)
        grad_c = jnp.zeros((CHUNK, states), F32)
        grad_b = jnp.zeros((CHUNK, states), F32)
        for pair in range(heads // 2):
            cols = slice(pair * LANES, (pair + 1) * LANES)
            gate = proj_ref[rows, cols]
            mixed = mixed_ref[rows, cols]
            gm = gm_ref[rows, cols].astype(F32)
            gain = chan_ref[1:2, cols]
            sig_gate = sigmoid(gate)
            silu_gate = gate * sig_gate
            gated = mixed * silu_gate
            normed = gated * inv
            mix_out_ref[rows, cols] = (normed * gain).astype(BF16)
            acc_chan_ref[0, :, cols] += fold_rows(gm * normed)
            grad_gated = inv * (gm * gain) - gated * pull
            grad_ref[rows, cols] = (
                grad_gated * mixed * (sig_gate * (1.0 + gate * (1.0 - sig_gate)))
            ).astype(BF16)
            gh = grad_gated * silu_gate
            x_pair = act[:, cols]
            x_wide = x_pair.astype(F32)
            acc_chan_ref[1, :, cols] += fold_rows(gh * x_wide)
            gh_low = gh.astype(BF16)
            parts = []
            for side in range(2):
                head = 2 * pair + side
                keep = half if side == 0 else jnp.logical_not(half)
                x_side = jnp.where(keep, x_wide, 0.0).astype(BF16)
                cross = mm(x_side, gh_low, NT)
                gap = jnp.where(upper, cum_t[head : head + 1, :] - cum[:, head : head + 1], FAR)
                decay = jnp.exp(gap)
                parts.append((scores_t * decay).astype(BF16))
                bare = decay * cross
                timed = bare * step[:, head : head + 1]
                grad_scores = grad_scores + timed
                plain_sum = jnp.where(
                    lane == head, jnp.sum(bare * scores_t, axis=1, keepdims=True), plain_sum
                )
                row_parts.append(jnp.sum(timed * scores_t, axis=0, keepdims=True))
            g_two = jnp.concatenate(
                [jnp.where(half, gh, 0.0).astype(BF16), jnp.where(half, 0.0, gh).astype(BF16)], axis=0
            )
            within = mm(jnp.concatenate(parts, axis=1), g_two)
            state_pair = state_low[cols, :]
            grad_pair = grad_low[cols, :]
            fg = from_grad[:, cols]
            grad_x = (
                spread(step, pair, half) * (within + spread(fade, pair, half) * fg)
                + chan_ref[0:1, cols] * gh
            )
            later[0:CHUNK, cols] = grad_x * slope[:, cols]
            pick = (chan_head + 2 * pair == iota((LANES, LANES), 1)).astype(BF16)
            both = jnp.concatenate([x_wide * fg, gh * from_state[:, cols]], axis=0)
            high = both.astype(BF16)
            sums = mm(high, pick) + mm((both - high.astype(F32)).astype(BF16), pick)
            in_sum = in_sum + sums[:CHUNK]
            out_sum = out_sum + sums[CHUNK:]
            grown = (gh * spread(grow, pair, half)).astype(BF16)
            weighted = (x_wide * spread(tail, pair, half)).astype(BF16)
            grad_c = grad_c + mm(grown, state_pair)
            grad_b = grad_b + mm(weighted, grad_pair)
            update = mm(grown, c_mat, TN)
            for side in range(2):
                head = 2 * pair + side
                place = pl.ds(pair * LANES + side * 64, 64)
                held = grad_state[place, :]
                old = state_low[pair * LANES + side * 64 : pair * LANES + side * 64 + 64, :]
                meet = jnp.sum(jnp.sum(held * old.astype(F32), axis=0, keepdims=True), axis=1, keepdims=True)
                const_row = jnp.where(lane_row == head, meet, const_row)
                grad_state[place, :] = (
                    held * total[:, head : head + 1] + update[side * 64 : side * 64 + 64, :]
                )
        scores_low = grad_scores.astype(BF16)
        grad_b = grad_b + mm(scores_low, c_mat)
        grad_c = grad_c + mm(scores_low, b_mat, TN)
        later[0:CHUNK, channels : channels + states] = grad_b * slope[:, channels : channels + states]
        later[0:CHUNK, channels + states :] = grad_c * slope[:, channels + states :]
        row_sum = jnp.concatenate(row_parts + [jnp.zeros((CHUNK - heads, CHUNK), F32)], axis=0).T
        plain_in = in_sum * fade
        timed_in = plain_in * step
        flow = row_sum - plain_sum * step + out_sum * grow - timed_in
        grad_log = (
            mm_full(upper_ones, flow)
            + jnp.sum(timed_in, axis=0, keepdims=True)
            + const_row * total
        )
        grad_step = plain_sum + plain_in + row_ref[1:2, :] * grad_log
        grad_dt = grad_step * sigmoid(dt_raw)
        grad_ref[rows, dt_at:] = grad_dt.astype(BF16)
        acc_row_ref[0] += fold_rows(grad_dt)
        acc_row_ref[1] += fold_rows(grad_log * log_step)
        conv_in = proj_ref[rows, channels:dt_at]
        grad_pre = later[0:CHUNK, :]
        grad_in = conv_ref[3:4, :] * grad_pre
        acc_conv_ref[3] += fold_rows(conv_in * grad_pre)
        acc_conv_ref[4] += fold_rows(grad_pre)
        for ahead in range(1, 4):
            moved = later[ahead : ahead + CHUNK, :]
            grad_in = grad_in + conv_ref[3 - ahead : 4 - ahead, :] * moved
            acc_conv_ref[3 - ahead] += fold_rows(conv_in * moved)
        grad_ref[rows, channels:dt_at] = grad_in.astype(BF16)
        later[CHUNK : CHUNK + 8, :] = later[0:8, :]


def whole(shape):
    return pl.BlockSpec(shape, lambda i: (0,) * len(shape))


def run_forward(hidden, weights, grad_rows, w_out, conv_rows, head_rows, chan_rows, heads, channels, states):
    length, width = hidden.shape
    cols = weights.shape[1]
    conv_cols = channels + 2 * states
    steps = length // STEP
    subs = STEP // CHUNK

    def by_rows(n):
        return pl.BlockSpec((STEP, n), lambda i: (i, 0))

    return pl.pallas_call(
        functools.partial(fwd_kernel, heads, channels, states),
        grid=(steps,),
        in_specs=[
            by_rows(width), whole(weights.shape), by_rows(width), whole(w_out.shape),
            whole(conv_rows.shape), whole(head_rows.shape), whole(chan_rows.shape),
        ],
        out_specs=[
            by_rows(cols), by_rows(conv_cols), by_rows(channels), by_rows(channels),
            pl.BlockSpec((8, STEP), lambda i: (0, i)),
            pl.BlockSpec((subs, channels, states), lambda i: (i, 0, 0)),
        ],
        out_shape=[
            jax.ShapeDtypeStruct((length, cols), F32),
            jax.ShapeDtypeStruct((length, conv_cols), F32),
            jax.ShapeDtypeStruct((length, channels), F32),
            jax.ShapeDtypeStruct((length, channels), BF16),
            jax.ShapeDtypeStruct((8, length), F32),
            jax.ShapeDtypeStruct((length // CHUNK, channels, states), BF16),
        ],
        scratch_shapes=[pltpu.VMEM((8 + STEP, conv_cols), F32), pltpu.VMEM((channels, states), F32)],
        compiler_params=pltpu.CompilerParams(dimension_semantics=("arbitrary",), vmem_limit_bytes=56 << 20),
        cost_estimate=pl.CostEstimate(
            flops=2 * length * width * (cols + channels) + length * heads * 60000,
            bytes_accessed=length * (width * 4 + cols * 4 + conv_cols * 4 + channels * 6),
            transcendentals=length * heads * 256,
        ),
        name="mixer_forward",
    )(hidden, weights, grad_rows, w_out, conv_rows, head_rows, chan_rows)


def run_backward(proj, pre, mixed, gm, stats, starts, conv_rows, head_rows, chan_rows, heads, channels, states, total_channels):
    length, cols = proj.shape
    conv_cols = channels + 2 * states
    steps = length // STEP
    subs = STEP // CHUNK

    def by_rows(n):
        return pl.BlockSpec((STEP, n), lambda i: (steps - 1 - i, 0))

    return pl.pallas_call(
        functools.partial(bwd_kernel, heads, channels, states, total_channels),
        grid=(steps,),
        in_specs=[
            by_rows(cols), by_rows(conv_cols), by_rows(channels), by_rows(channels),
            pl.BlockSpec((8, STEP), lambda i: (0, steps - 1 - i)),
            pl.BlockSpec((subs, channels, states), lambda i: (steps - 1 - i, 0, 0)),
            whole(conv_rows.shape), whole(head_rows.shape), whole(chan_rows.shape),
        ],
        out_specs=[
            by_rows(channels), by_rows(cols),
            whole((5, 8, conv_cols)), whole((2, 8, channels)), whole((2, 8, LANES)),
        ],
        out_shape=[
            jax.ShapeDtypeStruct((length, channels), BF16),
            jax.ShapeDtypeStruct((length, cols), BF16),
            jax.ShapeDtypeStruct((5, 8, conv_cols), F32),
            jax.ShapeDtypeStruct((2, 8, channels), F32),
            jax.ShapeDtypeStruct((2, 8, LANES), F32),
        ],
        scratch_shapes=[pltpu.VMEM((CHUNK + 8, conv_cols), F32), pltpu.VMEM((channels, states), F32)],
        compiler_params=pltpu.CompilerParams(dimension_semantics=("arbitrary",), vmem_limit_bytes=56 << 20),
        cost_estimate=pl.CostEstimate(
            flops=length * heads * 200000,
            bytes_accessed=length * (cols * 6 + conv_cols * 4 + channels * 8),
            transcendentals=length * heads * 256,
        ),
        name="mixer_backward",
    )(proj, pre, mixed, gm, stats, starts, conv_rows, head_rows, chan_rows)


def body(
    acts, grad_out, norm_gain, w_zx, w_bc, w_dt, w_out,
    conv_x, conv_x_bias, conv_bc, conv_bc_bias, dt_bias, a_log, d_skip, gate_gain,
):
    parts = lax.axis_size("tensor")
    rank = lax.axis_index("tensor")
    channels = w_zx.shape[2]
    heads = w_dt.shape[1]
    states = w_bc.shape[1] // 2
    head_width = channels // heads
    total_channels = channels * parts
    total_heads = heads * parts
    chan_start = rank * channels
    head_start = rank * heads
    shard = w_zx.shape[0]

    def mine(v, start, size):
        return lax.dynamic_slice_in_dim(v, start, size, v.ndim - 1)

    def pad_lanes(v):
        return jnp.pad(v, ((0, 0), (0, LANES - v.shape[1])))

    packed = jnp.concatenate([w_zx.reshape(shard, 2 * channels), w_bc, pad_lanes(w_dt)], axis=1)
    weights = lax.all_gather(packed, "dp", axis=0, tiled=True)
    out_full = lax.all_gather(w_out, "dp", axis=0, tiled=True)
    acts_row = acts[0].astype(F32)
    grad_row = grad_out[0]
    inv0 = lax.rsqrt(jnp.mean(acts_row * acts_row, axis=-1, keepdims=True) + EPSILON)
    hidden = lax.all_gather(
        (acts_row * inv0 * norm_gain).astype(BF16), "tensor", axis=0, tiled=True
    )
    grad_rows = lax.all_gather(grad_row, "tensor", axis=0, tiled=True)

    conv_rows = jnp.concatenate(
        [
            jnp.concatenate([mine(conv_x, chan_start, channels), conv_bc], axis=1),
            jnp.concatenate([mine(conv_x_bias, chan_start, channels), conv_bc_bias])[None],
            jnp.zeros((3, channels + 2 * states), F32),
        ],
        axis=0,
    )
    dt_bias_mine = mine(dt_bias, head_start, heads)
    rate_mine = -jnp.exp(mine(a_log, head_start, heads))
    head_rows = jnp.pad(jnp.stack([dt_bias_mine, rate_mine]), ((0, 6), (0, LANES - heads)))
    chan_rows = jnp.pad(
        jnp.stack(
            [jnp.repeat(mine(d_skip, head_start, heads), head_width), mine(gate_gain, chan_start, channels)]
        ),
        ((0, 6), (0, 0)),
    )
    proj, pre, mixed, gm, stats, starts = run_forward(
        hidden, weights, grad_rows, out_full, conv_rows, head_rows, chan_rows, heads, channels, states
    )
    stats = lax.psum(stats, "tensor")
    mixed_out, grads, acc_conv, acc_chan, acc_row = run_backward(
        proj, pre, mixed, gm, stats, starts, conv_rows, head_rows, chan_rows,
        heads, channels, states, total_channels,
    )
    projected = lax.psum_scatter(
        mm(mixed_out, out_full, NT).astype(BF16), "tensor", scatter_dimension=0, tiled=True
    )
    out_acts = (acts_row + projected.astype(F32)).astype(BF16)[None]
    grad_w_out = lax.psum_scatter(
        mm(grad_rows, mixed_out, TN).astype(BF16), "dp", scatter_dimension=0, tiled=True
    ).astype(F32)
    grad_hidden = lax.psum_scatter(
        mm(grads, weights, NT).astype(BF16), "tensor", scatter_dimension=0, tiled=True
    ).astype(F32)
    grad_weights = lax.psum_scatter(
        mm(hidden, grads, TN).astype(BF16), "dp", scatter_dimension=0, tiled=True
    ).astype(F32)
    grad_w_zx = grad_weights[:, : 2 * channels].reshape(shard, 2, channels)
    grad_w_dt = grad_weights[:, 2 * channels + 2 * states : 2 * channels + 2 * states + heads]
    grad_w_bc = lax.psum(grad_weights[:, 2 * channels : 2 * channels + 2 * states], "tensor")

    scaled = grad_hidden * norm_gain
    inner = jnp.sum(scaled * acts_row, axis=1, keepdims=True)
    grad_acts = (
        grad_row.astype(F32)
        + scaled * inv0
        - acts_row * (inv0 * inv0 * inv0 * (inner / acts_row.shape[1]))
    )[None]
    grad_ng = jnp.sum(grad_hidden * acts_row * inv0, axis=0)

    conv_sum = jnp.sum(acc_conv, axis=1)
    chan_sum = jnp.sum(acc_chan, axis=1)
    row_sum = jnp.sum(acc_row, axis=1)[:, :heads]
    skip_sum = jnp.sum(chan_sum[1].reshape(heads, head_width), axis=1)

    def widen(piece, start, size):
        holder = jnp.zeros(piece.shape[:-1] + (size,), F32)
        return lax.dynamic_update_slice_in_dim(holder, piece, start, piece.ndim - 1)

    wide = jnp.concatenate([conv_sum[:, :channels], chan_sum[0:1]], axis=0)
    head_sums = jnp.concatenate([row_sum, skip_sum[None]], axis=0)
    flat = jnp.concatenate(
        [
            grad_ng,
            widen(wide, chan_start, total_channels).reshape(-1),
            conv_sum[:, channels:].reshape(-1),
            widen(head_sums, head_start, total_heads).reshape(-1),
        ]
    )
    flat = lax.psum(flat, ("dp", "tensor"))
    at = 0
    pieces = []
    for shape in ((acts_row.shape[1],), (6, total_channels), (5, 2 * states), (3, total_heads)):
        size = 1
        for extent in shape:
            size *= extent
        pieces.append(flat[at : at + size].reshape(shape))
        at += size
    grad_ng, wide, conv_b, head_sums = pieces
    return (
        out_acts, grad_acts, grad_ng, grad_w_zx, grad_w_bc, grad_w_dt, grad_w_out,
        wide[:4], wide[4], conv_b[:4], conv_b[4],
        head_sums[0], head_sums[1], head_sums[2], wide[5],
    )


def solution(mesh):
    in_specs = (
        P("dp", "tensor", None), P("dp", "tensor", None), P(),
        P("dp", None, "tensor"), P("dp", None), P("dp", "tensor"), P("dp", "tensor"),
    ) + (P(),) * 8
    out_specs = (
        P("dp", "tensor", None), P("dp", "tensor", None), P(),
        P("dp", None, "tensor"), P("dp", None), P("dp", "tensor"), P("dp", "tensor"),
    ) + (P(),) * 8
    return jax.shard_map(body, mesh=mesh, in_specs=in_specs, out_specs=out_specs, check_vma=False)
```
